32 devices in a mesh: lat: 8 (over z, y), ch: 4 (over x, core).
Axes of the slice: x: 2, y: 2, z: 4, core: 2. Of those that a mesh axis runs over, the one named last changes fastest.
Arguments:
- field: bfloat16 [728, 256, 1440], P('lat', 'ch'), may hold values from -6 to 6
- legendre: bfloat16 [384, 721, 728], P(('lat', 'ch')), may hold values from -0.21875 to 0.21875
- pair_order: int32 [384], replicated, may hold values from 0 to 383, each once
Outputs:
- coeffs: float32 [384, 721, 2, 256], P(('lat', 'ch'))
The draws below stay inside these ranges and needn't reach their ends.
Inputs may be any that keep to these rules, and one draw needn't show every extreme that they name: `pair_order`: each of 0 to 383 appears once; a value p below 360 gives its bin the orders p and 719 - p, and a bin with a larger value is empty.
All inputs are finite; a program needn't handle non-finite values.
Results may differ from the reference program's by a relative error of at most 0.0037.
Values may be sent and summed in bfloat16 or wider, within the bound.
A program may use at most 256 MiB of HBM per device.

```python
import math
import jax
import jax.numpy as jnp
from jax import lax

NLAT = 721
NLON = 1440
C = 256
LMAX = 720
BINS = 384
LATP = 728
N_LAT = 8


def shard_levels(rng, shape, split, low, top_value):
    def one(dim, parts):
        draws = jax.random.uniform(jax.random.fold_in(jax.random.fold_in(rng, 6), dim), (parts,), jnp.float32, low / len(split), top_value / len(split))
        return jnp.repeat(jnp.exp(draws), shape[dim] // parts).reshape((-1,) + (1,) * (len(shape) - dim - 1))

    gain = one(*split[0])
    for cut in split[1:]:
        gain = gain * one(*cut)
    return gain


def noise(key, dims, width, limit, shards=(), held_as=jnp.bfloat16):
    result = width * jax.random.normal(key, dims, jnp.float32)
    if shards:
        result = result * shard_levels(key, dims, shards, -0.22, 0.18)
    return jnp.clip(result, -limit, limit).astype(held_as)


def setup_inputs(seed: int = 0) -> dict:
    keys = jax.random.split(jax.random.key(seed), 4)
    field = noise(keys[0], (LATP, C, NLON), 1.0, 6.0, ((0, 8), (1, 4)))
    legendre = noise(keys[1], (BINS, LMAX + 1, LATP), NLAT ** -0.5, 0.21875, ((0, 32),))
    pair_order = jax.random.permutation(keys[2], BINS).astype(jnp.int32)
    return {"field": field, "legendre": legendre, "pair_order": pair_order}


def dft_table(points, modes, lon_count):
    turns = (points[:, None] * modes[None, :]) % lon_count
    angle = turns.astype(jnp.float32) * (2.0 * math.pi / lon_count)
    return jnp.stack([jnp.cos(angle), -jnp.sin(angle)], axis=-1).astype(jnp.bfloat16)


def reference(field, legendre, pair_order):
    lat_total, chan_count, lon_count = field.shape
    max_order = legendre.shape[1] - 1
    lat_index = jnp.arange(lat_total, dtype=jnp.int32)
    masked = jnp.where((lat_index < NLAT)[:, None, None], field, jnp.zeros_like(field))
    dft_basis = dft_table(jnp.arange(lon_count, dtype=jnp.int32), jnp.arange(max_order, dtype=jnp.int32), lon_count)
    dft_basis = dft_basis.reshape(lon_count, 2 * max_order)
    norm_scale = 2.0 * math.pi / lon_count
    lat_blocks = masked.reshape(N_LAT, lat_total // N_LAT, chan_count, lon_count)

    def transform(lat_block):
        output = jnp.dot(lat_block.reshape(-1, lon_count), dft_basis, preferred_element_type=jnp.float32) * norm_scale
        return output.astype(jnp.bfloat16).reshape(lat_block.shape[0], chan_count, max_order, 2)

    fourier = lax.map(transform, lat_blocks).reshape(lat_total, chan_count, max_order, 2)
    keep_mask = pair_order < max_order // 2
    first_order = jnp.where(keep_mask, pair_order, 0).astype(jnp.int32)
    degree = jnp.arange(max_order + 1, dtype=jnp.int32)

    def one_slot(inputs):
        basis_rows, order_one, alive_flag = inputs
        order_two = (max_order - 1 - order_one).astype(jnp.int32)
        rows_one = lax.dynamic_index_in_dim(fourier, order_one, 2, keepdims=False)
        rows_two = lax.dynamic_index_in_dim(fourier, order_two, 2, keepdims=False)
        prod_one = jnp.dot(basis_rows, rows_one.reshape(lat_total, -1), preferred_element_type=jnp.float32)
        prod_two = jnp.dot(basis_rows, rows_two.reshape(lat_total, -1), preferred_element_type=jnp.float32)
        prod_one = prod_one.reshape(max_order + 1, chan_count, 2)
        prod_two = prod_two.reshape(max_order + 1, chan_count, 2)
        chosen = jnp.where((degree < max_order - order_one)[:, None, None], prod_one, prod_two)
        return jnp.transpose(chosen, (0, 2, 1)) * alive_flag.astype(jnp.float32)

    return lax.map(one_slot, (legendre, first_order, keep_mask))
```

```python
import functools
import math

import jax
import jax.numpy as jnp
import numpy as np
from jax import lax
from jax.experimental import pallas as pl
from jax.experimental.pallas import tpu as pltpu
from jax.sharding import PartitionSpec as P

NLAT = 721
PER = 2
DB = 32
LANES = 128
MESH = pl.DeviceIdType.MESH


def up(x, m):
    return -(-x // m) * m


def cos_coeffs():
    cheb = np.polynomial.chebyshev.Chebyshev.interpolate(
        lambda u: np.cos(np.pi * np.sqrt(np.abs(u))), 8, domain=[0.0, 1.0]
    )
    return [float(c) for c in cheb.convert(kind=np.polynomial.Polynomial).coef]


def xor(a, b, count):
    total, bit = 0, 1
    while bit < count:
        total = total + ((a // bit + b // bit) % 2) * bit
        bit *= 2
    return total


class Sizes:
    def __init__(self, field_shape, leg_shape, lat_count, ch_count):
        self.rows, self.chan, self.lon = field_shape
        self.own, self.deg, self.latp = leg_shape
        self.nl, self.nc = lat_count, ch_count
        self.nd = lat_count * ch_count
        self.orders = self.deg - 1
        self.groups = self.own // PER
        self.blocks = self.nd // DB
        self.step = max(s for s in range(1, 17) if self.rows % s == 0)
        self.chunks = self.rows // self.step
        self.clen = self.step * self.chan
        self.cpad = up(self.clen, LANES)
        self.pair = 2 * self.rows
        self.zrows = up(PER * self.pair, 16)
        self.start = [(b * self.pair) // 16 * 16 for b in range(PER)]
        self.win = max(
            [up((b + 1) * self.pair - self.start[b], 16) for b in range(PER)]
        )
        self.start = [min(s, self.zrows - self.win) for s in self.start]
        self.depth = self.nl * self.win
        self.ct = self.nc * self.chan // LANES
        self.per_row = 2 * self.ct
        self.orows = PER * self.deg * self.per_row


def kernel(
    z, field, leg, mcol, marks, bounds, out,
    fbuf, basis, zbuf, send, recv, sel, pbuf, obuf,
    fsem, psem, osem, send_sem, recv_sem,
):
    lat = lax.axis_index("lat")
    ch = lax.axis_index("ch")
    me = lat * z.nc + ch
    poly = cos_coeffs()
    scale = 2.0 * math.pi / z.lon
    total_steps = z.groups * z.chunks
    lane = lax.broadcasted_iota(jnp.int32, (1, LANES), 1)
    low = lane < LANES // 2

    def field_copy(n, slot):
        c = lax.rem(n, z.chunks)
        src = field.at[pl.ds(pl.multiple_of(c * z.clen, 16), z.clen)]
        return pltpu.make_async_copy(src, fbuf.at[slot, pl.ds(0, z.clen)], fsem.at[slot])

    field_copy(0, 0).start()

    def build_basis(g, blk):
        def one(s, _):
            m = mcol[g, pl.ds(pl.multiple_of(blk * 8 * DB + s * 16, 16), 16), :]
            phase = ((s // 2) % 2) * (z.lon // 4)
            k = lax.broadcasted_iota(jnp.int32, (16, z.lon), 1).astype(jnp.float32)
            x = m * k + phase.astype(jnp.float32)
            r = x - z.lon * jnp.floor(x * (1.0 / z.lon) + 0.5)
            r = r * (2.0 / z.lon)
            u = r * r
            acc = jnp.full_like(u, poly[-1])
            for c in poly[-2::-1]:
                acc = acc * u + c
            basis[blk, pl.ds(pl.multiple_of(s * 16, 16), 16), :] = acc.astype(jnp.bfloat16)
            return 0

        lax.fori_loop(0, 8 * DB // 16, one, 0)

    def transform(g):
        def chunk(c, _):
            n = g * z.chunks + c
            slot = lax.rem(n, 2)

            @pl.when(n + 1 < total_steps)
            def _():
                field_copy(n + 1, lax.rem(n + 1, 2)).start()

            @pl.when(c == 0)
            def _():
                lax.fori_loop(0, z.blocks, lambda blk, _: (build_basis(g, blk), 0)[1], 0)

            field_copy(n, slot).wait()

            def block(blk, _):
                ft = lax.dot_general(
                    basis[blk], fbuf[slot], (((1,), (1,)), ((), ())),
                    preferred_element_type=jnp.float32,
                )
                for s in range(2 * PER):
                    re = ft[2 * s * DB : (2 * s + 1) * DB]
                    im = ft[(2 * s + 1) * DB : (2 * s + 2) * DB]
                    for j in range(z.cpad // LANES):
                        v0 = re[:, j * LANES : (j + 1) * LANES]
                        v1 = im[:, j * LANES : (j + 1) * LANES]
                        base = blk * DB * z.zrows + s * z.rows + c * z.step + 2 * j
                        even = jnp.where(low, v0, pltpu.roll(v1, LANES // 2, 1))
                        zbuf[pl.ds(base, DB, stride=z.zrows), :] = even
                        if 2 * j + 1 < z.step:
                            odd = jnp.where(low, pltpu.roll(v0, LANES // 2, 1), v1)
                            zbuf[pl.ds(base + 1, DB, stride=z.zrows), :] = odd
                return 0

            lax.fori_loop(0, z.blocks, block, 0)
            return 0

        lax.fori_loop(0, z.chunks, chunk, 0)

    def all_sent(slot):
        ref = send.at[slot, pl.ds(0, z.nd - 1)]
        return pltpu.make_async_copy(ref, ref, send_sem.at[slot])

    def all_here(g):
        ref = send.at[0, pl.ds(0, z.nd - 1)]
        return pltpu.make_async_copy(ref, ref, recv_sem.at[g])

    def pack_and_send(g):
        slot = lax.rem(g, 2)

        def pack(d, _):
            rows = zbuf[pl.ds(pl.multiple_of(d * z.zrows, 16), z.zrows), :]
            send[slot, d] = (rows * scale).astype(jnp.bfloat16)
            return 0

        lax.fori_loop(0, z.nd, pack, 0)

        def issue(n, _):
            d = xor(me, z.nd - 1 - n, z.nd)
            pltpu.make_async_remote_copy(
                src_ref=send.at[slot, d],
                dst_ref=recv.at[g, lat, ch],
                send_sem=send_sem.at[slot],
                recv_sem=recv_sem.at[g],
                device_id=(d // z.nc, d % z.nc),
                device_id_type=MESH,
            ).start()
            return 0

        lax.fori_loop(0, z.nd - 1, issue, 0)
        recv[g, lat, ch] = send[slot, me]

    def leg_copy(g, b):
        return pltpu.make_async_copy(leg.at[g * PER + b], pbuf.at[b], psem.at[b])

    def build_select():
        step = max(s for s in range(8, 129, 8) if z.latp % s == 0)
        for b in range(PER):
            target = marks[b, 0:1, :]

            def one(n, _):
                at = pl.multiple_of(n * step, 8)
                row = lax.broadcasted_iota(jnp.int32, (step, 1), 0) + at
                hit = jnp.where(row == target, 1.0, 0.0).astype(jnp.bfloat16)
                sel[b, pl.ds(at, step), :] = hit
                return 0

            lax.fori_loop(0, z.latp // step, one, 0)

    cuts = [0, 240, 480, z.deg]

    def out_copy(g):
        dst = out.at[pl.ds(pl.multiple_of(g * z.orows, 8), z.orows)]
        return pltpu.make_async_copy(obuf, dst, osem)

    def legendre(g):
        all_here(g).wait()
        for b in range(PER):
            leg_copy(g, b).wait()
            first = bounds[0, g * PER + b]
            second = bounds[1, g * PER + b]
            in_first = marks[b, 1:2, :] == 0
            at = z.start[b]
            rhs = jnp.concatenate(
                [
                    recv[g, :, j, at : at + z.win, :].reshape(z.depth, LANES)
                    for j in range(z.nc)
                ],
                axis=1,
            )
            for lo, hi in zip(cuts[:-1], cuts[1:]):
                spread = jnp.dot(
                    pbuf[b, lo:hi, :], sel[b], preferred_element_type=jnp.float32
                )
                r = lax.broadcasted_iota(jnp.int32, (hi - lo, 1), 0) + lo
                upper = jnp.where(r < first, 1.0, 0.0)
                lower = jnp.where(r >= second, 1.0, 0.0)
                mask = jnp.where(in_first, upper, lower)
                lhs = (spread * mask).astype(jnp.bfloat16)
                y = jnp.dot(lhs, rhs, preferred_element_type=jnp.float32)
                for t in range(z.ct):
                    p0 = y[:, 2 * t * LANES : (2 * t + 1) * LANES]
                    p1 = y[:, (2 * t + 1) * LANES : (2 * t + 2) * LANES]
                    re = jnp.where(low, p0, pltpu.roll(p1, LANES // 2, 1))
                    im = jnp.where(low, pltpu.roll(p0, LANES // 2, 1), p1)
                    base = (b * z.deg + lo) * z.per_row + 2 * t
                    obuf[pl.ds(base, hi - lo, stride=z.per_row), :] = re
                    obuf[pl.ds(base + 1, hi - lo, stride=z.per_row), :] = im
        out_copy(g).start()
        out_copy(g).wait()

    def body(g, _):
        @pl.when(g < z.groups)
        def _():
            @pl.when(g == 0)
            def _():
                zbuf[...] = jnp.zeros_like(zbuf)

            transform(g)

            @pl.when(g >= 2)
            def _():
                all_sent(lax.rem(g, 2)).wait()

            pack_and_send(g)

            @pl.when(g == 0)
            def _():
                build_select()

        @pl.when(g >= 2)
        def _():
            for b in range(PER):
                leg_copy(g - 2, b).start()
            legendre(g - 2)

        return 0

    lax.fori_loop(0, z.groups + 2, body, 0)
    for g in range(max(z.groups - 2, 0), z.groups):
        all_sent(g % 2).wait()


def per_device(field, legendre, pair_order):
    z = Sizes(
        field.shape, legendre.shape, lax.axis_size("lat"), lax.axis_size("ch")
    )
    me = lax.axis_index("lat") * z.nc + lax.axis_index("ch")
    keep = pair_order < z.orders // 2
    first = jnp.where(keep, pair_order, 0)
    both = jnp.stack([first, z.orders - 1 - first], axis=1)
    cols = both.reshape(z.blocks, DB, z.groups, PER, 2).transpose(2, 0, 3, 4, 1)
    cols = jnp.broadcast_to(cols[:, :, :, :, None, :], cols.shape[:4] + (2, DB))
    mcol = cols.reshape(z.groups, z.blocks * 8 * DB, 1).astype(jnp.float32)
    far = 4 * z.deg
    lims = jnp.stack(
        [jnp.where(keep, z.orders - first, 0), jnp.where(keep, z.orders - first, far)]
    )
    bounds = lax.dynamic_slice_in_dim(lims, me * z.own, z.own, axis=1)

    col = np.arange(z.depth)
    marks = np.zeros((PER, 8, z.depth), np.int32)
    for b in range(PER):
        u = col % z.win - (b * z.pair - z.start[b])
        lat = (col // z.win) * z.rows + u % z.rows
        ok = (u >= 0) & (u < z.pair) & (lat < NLAT)
        marks[b, 0] = np.where(ok, lat, -1)
        marks[b, 1] = (u // z.rows) % 2

    bf, f32 = jnp.bfloat16, jnp.float32
    vmem = pl.BlockSpec(memory_space=pltpu.VMEM)
    hbm = pl.BlockSpec(memory_space=pl.ANY)
    dma = pltpu.SemaphoreType.DMA
    flat = pl.pallas_call(
        functools.partial(kernel, z),
        out_shape=jax.ShapeDtypeStruct((z.groups * z.orows, LANES), f32),
        in_specs=[hbm, hbm, vmem, vmem, pl.BlockSpec(memory_space=pltpu.SMEM)],
        out_specs=hbm,
        scratch_shapes=[
            pltpu.VMEM((2, z.cpad, z.lon), bf),
            pltpu.VMEM((z.blocks, 8 * DB, z.lon), bf),
            pltpu.VMEM((z.nd * z.zrows, LANES), f32),
            pltpu.VMEM((2, z.nd, z.zrows, LANES), bf),
            pltpu.VMEM((z.groups, z.nl, z.nc, z.zrows, LANES), bf),
            pltpu.VMEM((PER, z.latp, z.depth), bf),
            pltpu.VMEM((PER, z.deg, z.latp), bf),
            pltpu.VMEM((z.orows, LANES), f32),
            dma((2,)), dma((PER,)), dma, dma((2,)), dma((z.groups,)),
        ],
        compiler_params=pltpu.CompilerParams(
            has_side_effects=True, vmem_limit_bytes=67043328
        ),
    )(
        field.reshape(z.rows * z.chan, z.lon), legendre, mcol, jnp.asarray(marks), bounds
    )
    shaped = flat.reshape(z.own, z.deg, z.ct, 2, LANES).transpose(0, 1, 3, 2, 4)
    return shaped.reshape(z.own, z.deg, 2, z.ct * LANES)


def solution(mesh):
    in_specs = (P("lat", "ch", None), P(("lat", "ch"), None, None), P())
    out_specs = P(("lat", "ch"), None, None, None)
    return jax.shard_map(
        per_device, mesh=mesh, in_specs=in_specs, out_specs=out_specs, check_vma=False
    )
```

```python
import functools
import math

import jax
import jax.numpy as jnp
import numpy as np
from jax import lax
from jax.experimental import pallas as pl
from jax.experimental.pallas import tpu as pltpu
from jax.sharding import PartitionSpec as P

NLAT = 721
PER = 2
DB = 32
LANES = 128
MESH = pl.DeviceIdType.MESH


def up(x, m):
    return -(-x // m) * m


def cos_coeffs():
    cheb = np.polynomial.chebyshev.Chebyshev.interpolate(
        lambda u: np.cos(np.pi * np.sqrt(np.abs(u))), 8, domain=[0.0, 1.0]
    )
    return [float(c) for c in cheb.convert(kind=np.polynomial.Polynomial).coef]


def xor(a, b, count):
    total, bit = 0, 1
    while bit < count:
        total = total + ((a // bit + b // bit) % 2) * bit
        bit *= 2
    return total


class Sizes:
    def __init__(self, field_shape, leg_shape, lat_count, ch_count):
        self.rows, self.chan, self.lon = field_shape
        self.own, self.deg, self.latp = leg_shape
        self.nl, self.nc = lat_count, ch_count
        self.nd = lat_count * ch_count
        self.orders = self.deg - 1
        self.groups = self.own // PER
        self.blocks = self.nd // DB
        self.step = max(s for s in range(1, 9) if self.rows % s == 0)
        self.chunks = self.rows // self.step
        self.clen = self.step * self.chan
        self.cpad = up(self.clen, LANES)
        self.pair = 2 * self.rows
        self.zrows = up(PER * self.pair, 16)
        self.start = [(b * self.pair) // 16 * 16 for b in range(PER)]
        self.win = max(
            [up((b + 1) * self.pair - self.start[b], 16) for b in range(PER)]
        )
        self.start = [min(s, self.zrows - self.win) for s in self.start]
        self.depth = self.nl * self.win
        mid = up(self.zrows // 2, 16)
        self.pieces = [(0, mid), (mid, self.zrows - mid)]
        self.ct = self.nc * self.chan // LANES
        self.per_row = 2 * self.ct
        self.orows = PER * self.deg * self.per_row


def kernel(
    z, field, leg, mrow, marks, bounds, out,
    fbuf, basis, zbuf, send, recv, sel, pbuf, lhs,
    fsem, psem, send_sem, recv_sem,
):
    lat = lax.axis_index("lat")
    ch = lax.axis_index("ch")
    me = lat * z.nc + ch
    poly = cos_coeffs()
    scale = 2.0 * math.pi / z.lon
    total_steps = z.groups * z.chunks
    lane = lax.broadcasted_iota(jnp.int32, (1, LANES), 1)
    low = lane < LANES // 2

    def field_copy(n, slot):
        c = lax.rem(n, z.chunks)
        src = field.at[pl.ds(pl.multiple_of(c * z.clen, 16), z.clen)]
        return pltpu.make_async_copy(src, fbuf.at[slot, pl.ds(0, z.clen)], fsem.at[slot])

    field_copy(0, 0).start()

    def partner(n):
        i = n // 2
        t = z.nd - 1 - i // 2 - (z.nd // 4) * (i % 2) - (z.nd // 2) * (n % 2)
        return xor(me, t, z.nd)

    barrier = pltpu.get_barrier_semaphore()

    def greet(n, _):
        d = partner(n)
        pl.semaphore_signal(
            barrier, inc=1, device_id=(d // z.nc, d % z.nc), device_id_type=MESH
        )
        return 0

    lax.fori_loop(0, z.nd - 1, greet, 0)

    tall = max(s for s in range(16, 97, 16) if z.lon % s == 0)

    def build_basis(g, blk):
        at = pl.multiple_of(blk * 8 * DB, LANES)
        m = mrow[g, 0:1, pl.ds(at, 8 * DB)]
        phase = mrow[g, 1:2, pl.ds(at, 8 * DB)]

        def one(s, _):
            top = pl.multiple_of(s * tall, 16)
            k = lax.broadcasted_iota(jnp.int32, (tall, 8 * DB), 0) + top
            x = m * k.astype(jnp.float32) + phase
            r = x - z.lon * jnp.floor(x * (1.0 / z.lon) + 0.5)
            r = r * (2.0 / z.lon)
            u = r * r
            acc = jnp.full_like(u, poly[-1])
            for c in poly[-2::-1]:
                acc = acc * u + c
            basis[blk, pl.ds(top, tall), :] = acc.astype(jnp.bfloat16)
            return 0

        lax.fori_loop(0, z.lon // tall, one, 0)

    def transform(g):
        def chunk(c, _):
            n = g * z.chunks + c
            slot = lax.rem(n, 2)

            @pl.when(n + 1 < total_steps)
            def _():
                field_copy(n + 1, lax.rem(n + 1, 2)).start()

            @pl.when(c == 0)
            def _():
                lax.fori_loop(0, z.blocks, lambda blk, _: (build_basis(g, blk), 0)[1], 0)

            field_copy(n, slot).wait()

            def block(blk, _):
                ft = jnp.dot(fbuf[slot], basis[blk], preferred_element_type=jnp.float32)
                for j in range(z.cpad // LANES):
                    turned = jnp.transpose(ft[j * LANES : (j + 1) * LANES])
                    for s in range(2 * PER):
                        v0 = turned[2 * s * DB : (2 * s + 1) * DB]
                        v1 = turned[(2 * s + 1) * DB : (2 * s + 2) * DB]
                        base = blk * DB * z.zrows + s * z.rows + c * z.step + 2 * j
                        even = jnp.where(low, v0, pltpu.roll(v1, LANES // 2, 1))
                        zbuf[pl.ds(base, DB, stride=z.zrows), :] = even
                        if 2 * j + 1 < z.step:
                            odd = jnp.where(low, pltpu.roll(v0, LANES // 2, 1), v1)
                            zbuf[pl.ds(base + 1, DB, stride=z.zrows), :] = odd
                return 0

            lax.fori_loop(0, z.blocks, block, 0)
            return 0

        lax.fori_loop(0, z.chunks, chunk, 0)

    def clear_pads():
        def one(d, _):
            at = pl.multiple_of((d + 1) * z.zrows - 16, 16)
            zbuf[pl.ds(at, 16), :] = jnp.zeros((16, LANES), jnp.float32)
            return 0

        lax.fori_loop(0, z.nd, one, 0)

    def all_sent(slot):
        ref = send.at[slot, pl.ds(0, z.nd - 1)]
        return pltpu.make_async_copy(ref, ref, send_sem.at[slot])

    def all_here(g, piece):
        ref = send.at[0, pl.ds(0, z.nd - 1), pl.ds(*z.pieces[piece])]
        return pltpu.make_async_copy(ref, ref, recv_sem.at[g, piece])

    def pack(g):
        slot = lax.rem(g, 2)

        def one(d, _):
            rows = zbuf[pl.ds(pl.multiple_of(d * z.zrows, 16), z.zrows), :]
            send[slot, d] = (rows * scale).astype(jnp.bfloat16)
            return 0

        lax.fori_loop(0, z.nd, one, 0)

    def ship(g):
        slot = lax.rem(g, 2)
        for piece, (at, size) in enumerate(z.pieces):

            def issue(n, _):
                d = partner(n)
                pltpu.make_async_remote_copy(
                    src_ref=send.at[slot, d, pl.ds(at, size)],
                    dst_ref=recv.at[g, lat, ch, pl.ds(at, size)],
                    send_sem=send_sem.at[slot],
                    recv_sem=recv_sem.at[g, piece],
                    device_id=(d // z.nc, d % z.nc),
                    device_id_type=MESH,
                ).start()
                return 0

            lax.fori_loop(0, z.nd - 1, issue, 0)
        recv[g, lat, ch] = send[slot, me]

    def leg_copy(g, b):
        return pltpu.make_async_copy(leg.at[g * PER + b], pbuf, psem)

    tile = max(s for s in range(8, 129, 8) if z.latp % s == 0)

    def build_select(b):
        target = marks[b, 0:1, :]

        def one(n, _):
            at = pl.multiple_of(n * tile, 8)
            row = lax.broadcasted_iota(jnp.int32, (tile, 1), 0) + at
            hit = jnp.where(row == target, 1.0, 0.0).astype(jnp.bfloat16)
            sel[pl.ds(at, tile), :] = hit
            return 0

        lax.fori_loop(0, z.latp // tile, one, 0)

    cuts = [0, 240, 480, z.deg]
    spans = list(zip(cuts[:-1], cuts[1:]))

    def left_factor(g, b):
        build_select(b)
        leg_copy(g, b).wait()
        first = bounds[0, g * PER + b]
        second = bounds[1, g * PER + b]
        in_first = marks[b, 1:2, :] == 0
        for lo, hi in spans:
            spread = jnp.dot(pbuf[lo:hi, :], sel[...], preferred_element_type=jnp.float32)
            r = lax.broadcasted_iota(jnp.int32, (hi - lo, 1), 0) + lo
            upper = jnp.where(r < first, 1.0, 0.0)
            lower = jnp.where(r >= second, 1.0, 0.0)
            mask = jnp.where(in_first, upper, lower)
            lhs[b, lo:hi, :] = (spread * mask).astype(jnp.bfloat16)

    def product(g, b):
        at = z.start[b]
        rhs = jnp.concatenate(
            [
                recv[g, :, j, at : at + z.win, :].reshape(z.depth, LANES)
                for j in range(z.nc)
            ],
            axis=1,
        )
        for lo, hi in spans:
            y = jnp.dot(lhs[b, lo:hi, :], rhs, preferred_element_type=jnp.float32)
            for t in range(z.ct):
                p0 = y[:, 2 * t * LANES : (2 * t + 1) * LANES]
                p1 = y[:, (2 * t + 1) * LANES : (2 * t + 2) * LANES]
                re = jnp.where(low, p0, pltpu.roll(p1, LANES // 2, 1))
                im = jnp.where(low, pltpu.roll(p0, LANES // 2, 1), p1)
                base = g * z.orows + (b * z.deg + lo) * z.per_row + 2 * t
                out[pl.ds(base, hi - lo, stride=z.per_row), :] = re
                out[pl.ds(base + 1, hi - lo, stride=z.per_row), :] = im

    def body(g, _):
        @pl.when(g < z.groups)
        def _():
            @pl.when(g == 0)
            def _():
                clear_pads()

            transform(g)

            @pl.when(g >= 2)
            def _():
                all_sent(lax.rem(g, 2)).wait()

            pack(g)

            @pl.when(g == 0)
            def _():
                pl.semaphore_wait(barrier, z.nd - 1)

            ship(g)

        @pl.when(g >= 2)
        def _():
            for b in range(PER):
                leg_copy(g - 2, b).start()
                left_factor(g - 2, b)
            for b in range(PER):
                all_here(g - 2, b).wait()
                product(g - 2, b)

        return 0

    lax.fori_loop(0, z.groups + 2, body, 0)
    for g in range(max(z.groups - 2, 0), z.groups):
        all_sent(g % 2).wait()


def per_device(field, legendre, pair_order):
    z = Sizes(
        field.shape, legendre.shape, lax.axis_size("lat"), lax.axis_size("ch")
    )
    me = lax.axis_index("lat") * z.nc + lax.axis_index("ch")
    keep = pair_order < z.orders // 2
    first = jnp.where(keep, pair_order, 0)
    both = jnp.stack([first, z.orders - 1 - first], axis=1)
    cols = both.reshape(z.blocks, DB, z.groups, PER, 2).transpose(2, 0, 3, 4, 1)
    cols = jnp.broadcast_to(cols[:, :, :, :, None, :], cols.shape[:4] + (2, DB))
    cols = cols.reshape(z.groups, z.blocks * 8 * DB).astype(jnp.float32)
    turn = np.arange(z.blocks * 8 * DB) // DB % 2 * (z.lon // 4)
    turn = jnp.broadcast_to(jnp.asarray(turn, jnp.float32), cols.shape)
    mrow = jnp.stack([cols, turn], axis=1)
    far = 4 * z.deg
    lims = jnp.stack(
        [jnp.where(keep, z.orders - first, 0), jnp.where(keep, z.orders - first, far)]
    )
    bounds = lax.dynamic_slice_in_dim(lims, me * z.own, z.own, axis=1)

    col = np.arange(z.depth)
    marks = np.zeros((PER, 8, z.depth), np.int32)
    for b in range(PER):
        u = col % z.win - (b * z.pair - z.start[b])
        lat = (col // z.win) * z.rows + u % z.rows
        ok = (u >= 0) & (u < z.pair) & (lat < NLAT)
        marks[b, 0] = np.where(ok, lat, -1)
        marks[b, 1] = (u // z.rows) % 2

    bf, f32 = jnp.bfloat16, jnp.float32
    vmem = pl.BlockSpec(memory_space=pltpu.VMEM)
    hbm = pl.BlockSpec(memory_space=pl.ANY)
    dma = pltpu.SemaphoreType.DMA
    flat = pl.pallas_call(
        functools.partial(kernel, z),
        out_shape=pltpu.VMEM((z.groups * z.orows, LANES), f32),
        in_specs=[hbm, hbm, vmem, vmem, pl.BlockSpec(memory_space=pltpu.SMEM)],
        out_specs=vmem,
        scratch_shapes=[
            pltpu.VMEM((2, z.cpad, z.lon), bf),
            pltpu.VMEM((z.blocks, z.lon, 8 * DB), bf),
            pltpu.VMEM((z.nd * z.zrows, LANES), f32),
            pltpu.VMEM((2, z.nd, z.zrows, LANES), bf),
            pltpu.VMEM((z.groups, z.nl, z.nc, z.zrows, LANES), bf),
            pltpu.VMEM((z.latp, z.depth), bf),
            pltpu.VMEM((z.deg, z.latp), bf),
            pltpu.VMEM((PER, z.deg, z.depth), bf),
            dma((2,)), dma, dma((2,)), dma((z.groups, len(z.pieces))),
        ],
        compiler_params=pltpu.CompilerParams(
            collective_id=0, has_side_effects=True, vmem_limit_bytes=67043328 - 4 * LANES * z.groups * z.orows - (1 << 19)
        ),
    )(
        field.reshape(z.rows * z.chan, z.lon), legendre, mrow, jnp.asarray(marks), bounds
    )
    shaped = flat.reshape(z.own, z.deg, z.ct, 2, LANES).transpose(0, 1, 3, 2, 4)
    return shaped.reshape(z.own, z.deg, 2, z.ct * LANES)


def solution(mesh):
    in_specs = (P("lat", "ch", None), P(("lat", "ch"), None, None), P())
    out_specs = P(("lat", "ch"), None, None, None)
    return jax.shard_map(
        per_device, mesh=mesh, in_specs=in_specs, out_specs=out_specs, check_vma=False
    )
```

```python
import functools
import math

import jax
import jax.numpy as jnp
import numpy as np
from jax import lax
from jax.experimental import pallas as pl
from jax.experimental.pallas import tpu as pltpu
from jax.sharding import PartitionSpec as P

NLAT = 721
PER = 2
DB = 32
SLOTS = 3
STEP = 13
LANES = 128
MESH = pl.DeviceIdType.MESH


def up(x, m):
    return -(-x // m) * m


def cos_coeffs():
    cheb = np.polynomial.chebyshev.Chebyshev.interpolate(
        lambda u: np.cos(np.pi * np.sqrt(np.abs(u))), 8, domain=[0.0, 1.0]
    )
    return [float(c) for c in cheb.convert(kind=np.polynomial.Polynomial).coef]


def xor(a, b, count):
    total, bit = 0, 1
    while bit < count:
        total = total + ((a // bit + b // bit) % 2) * bit
        bit *= 2
    return total


class Sizes:
    def __init__(self, field_shape, leg_shape, lat_count, ch_count):
        self.rows, self.chan, self.lon = field_shape
        self.own, self.deg, self.latp = leg_shape
        self.nl, self.nc = lat_count, ch_count
        self.nd = lat_count * ch_count
        self.orders = self.deg - 1
        self.groups = self.own // PER
        self.blocks = self.nd // DB
        self.step = max(s for s in range(1, STEP + 1) if self.rows % s == 0)
        self.chunks = self.rows // self.step
        self.clen = self.step * self.chan
        self.cpad = up(self.clen, LANES)
        self.pair = 2 * self.rows
        self.zrows = up(PER * self.pair, 16)
        self.start = [(b * self.pair) // 16 * 16 for b in range(PER)]
        self.win = max(
            [up((b + 1) * self.pair - self.start[b], 16) for b in range(PER)]
        )
        self.start = [min(s, self.zrows - self.win) for s in self.start]
        self.depth = self.nl * self.win
        mid = up(self.zrows // 2, 16)
        self.pieces = [(0, mid), (mid, self.zrows - mid)]
        self.sends = []
        for piece, (at, size) in enumerate(self.pieces):
            part = up(size, 32) // 2
            self.sends += [(piece, at, part), (piece, at + part, size - part)]
        self.sends = [send for send in self.sends if send[2] > 0]
        self.ct = self.nc * self.chan // LANES
        self.per_row = 2 * self.ct
        self.orows = PER * self.deg * self.per_row


def kernel(
    z, field, leg, held, marks, order, out,
    fbuf, basis, zbuf, send, recv, sel, pbuf, lhs,
    fsem, psem, send_sem, recv_sem,
):
    lat = lax.axis_index("lat")
    ch = lax.axis_index("ch")
    me = lat * z.nc + ch
    poly = cos_coeffs()
    scale = 2.0 * math.pi / z.lon
    total_steps = z.groups * z.chunks
    lane = lax.broadcasted_iota(jnp.int32, (1, LANES), 1)
    low = lane < LANES // 2

    def field_copy(n, slot):
        c = lax.rem(n, z.chunks)
        src = field.at[pl.ds(pl.multiple_of(c * z.clen, 16), z.clen)]
        return pltpu.make_async_copy(src, fbuf.at[slot, pl.ds(0, z.clen)], fsem.at[slot])

    for n in range(min(SLOTS - 1, total_steps)):
        field_copy(n, n).start()

    def partner(n):
        i = n // 2
        t = z.nd - 1 - i // 2 - (z.nd // 4) * (i % 2) - (z.nd // 2) * (n % 2)
        return xor(me, t, z.nd)

    barrier = pltpu.get_barrier_semaphore()

    def greet(n, _):
        d = partner(n)
        pl.semaphore_signal(
            barrier, inc=1, device_id=(d // z.nc, d % z.nc), device_id_type=MESH
        )
        return 0

    lax.fori_loop(0, z.nd - 1, greet, 0)

    tall = max(s for s in range(16, 97, 16) if z.lon % s == 0)

    def build_basis(g, blk):
        at = pl.multiple_of(blk * 8 * DB, LANES)
        col = lax.broadcasted_iota(jnp.int32, (1, 8 * DB), 1)
        low_order = held[g, 0:1, pl.ds(at, 8 * DB)]
        low_order = jnp.where(low_order < z.orders // 2, low_order, 0)
        half = (col // (2 * DB)) % 2
        m = jnp.where(half == 0, low_order, z.orders - 1 - low_order).astype(jnp.float32)
        phase = (((col // DB) % 2) * (z.lon // 4)).astype(jnp.float32)

        def one(s, _):
            top = pl.multiple_of(s * tall, 16)
            k = lax.broadcasted_iota(jnp.int32, (tall, 8 * DB), 0) + top
            x = m * k.astype(jnp.float32) + phase
            r = x - z.lon * jnp.floor(x * (1.0 / z.lon) + 0.5)
            r = r * (2.0 / z.lon)
            u = r * r
            acc = jnp.full_like(u, poly[-1])
            for c in poly[-2::-1]:
                acc = acc * u + c
            basis[blk, pl.ds(top, tall), :] = acc.astype(jnp.bfloat16)
            return 0

        lax.fori_loop(0, z.lon // tall, one, 0)

    def transform(g):
        def chunk(c, _):
            n = g * z.chunks + c
            slot = lax.rem(n, SLOTS)
            ahead = n + SLOTS - 1

            @pl.when(ahead < total_steps)
            def _():
                field_copy(ahead, lax.rem(ahead, SLOTS)).start()

            @pl.when(c == 0)
            def _():
                lax.fori_loop(0, z.blocks, lambda blk, _: (build_basis(g, blk), 0)[1], 0)

            field_copy(n, slot).wait()

            def block(blk, _):
                ft = jnp.dot(fbuf[slot], basis[blk], preferred_element_type=jnp.float32)
                for j in range(z.cpad // LANES):
                    turned = jnp.transpose(ft[j * LANES : (j + 1) * LANES])
                    for s in range(2 * PER):
                        v0 = turned[2 * s * DB : (2 * s + 1) * DB]
                        v1 = turned[(2 * s + 1) * DB : (2 * s + 2) * DB]
                        base = blk * DB * z.zrows + s * z.rows + c * z.step + 2 * j
                        even = jnp.where(low, v0, pltpu.roll(v1, LANES // 2, 1))
                        zbuf[pl.ds(base, DB, stride=z.zrows), :] = even
                        if 2 * j + 1 < z.step:
                            odd = jnp.where(low, pltpu.roll(v0, LANES // 2, 1), v1)
                            zbuf[pl.ds(base + 1, DB, stride=z.zrows), :] = odd
                return 0

            lax.fori_loop(0, z.blocks, block, 0)
            return 0

        lax.fori_loop(0, z.chunks, chunk, 0)

    def clear_pads():
        def one(d, _):
            at = pl.multiple_of((d + 1) * z.zrows - 16, 16)
            zbuf[pl.ds(at, 16), :] = jnp.zeros((16, LANES), jnp.float32)
            return 0

        lax.fori_loop(0, z.nd, one, 0)

    def all_sent(slot):
        ref = send.at[slot, pl.ds(0, z.nd - 1)]
        return pltpu.make_async_copy(ref, ref, send_sem.at[slot])

    def all_here(g, piece):
        ref = send.at[0, pl.ds(0, z.nd - 1), pl.ds(*z.pieces[piece])]
        return pltpu.make_async_copy(ref, ref, recv_sem.at[g, piece])

    def pack(g):
        slot = lax.rem(g, 2)

        def one(d, _):
            rows = zbuf[pl.ds(pl.multiple_of(d * z.zrows, 16), z.zrows), :]
            send[slot, d] = (rows * scale).astype(jnp.bfloat16)
            return 0

        lax.fori_loop(0, z.nd, one, 0)

    def ship(g):
        slot = lax.rem(g, 2)
        for piece, at, size in z.sends:

            def issue(n, _):
                d = partner(n)
                pltpu.make_async_remote_copy(
                    src_ref=send.at[slot, d, pl.ds(at, size)],
                    dst_ref=recv.at[g, lat, ch, pl.ds(at, size)],
                    send_sem=send_sem.at[slot],
                    recv_sem=recv_sem.at[g, piece],
                    device_id=(d // z.nc, d % z.nc),
                    device_id_type=MESH,
                ).start()
                return 0

            lax.fori_loop(0, z.nd - 1, issue, 0)
        recv[g, lat, ch] = send[slot, me]

    def leg_copy(g, b):
        return pltpu.make_async_copy(leg.at[g * PER + b], pbuf, psem)

    tile = max(s for s in range(8, 129, 8) if z.latp % s == 0)

    def build_select(b):
        target = marks[b, 0:1, :]

        def one(n, _):
            at = pl.multiple_of(n * tile, 8)
            row = lax.broadcasted_iota(jnp.int32, (tile, 1), 0) + at
            hit = jnp.where(row == target, 1.0, 0.0).astype(jnp.bfloat16)
            sel[pl.ds(at, tile), :] = hit
            return 0

        lax.fori_loop(0, z.latp // tile, one, 0)

    cuts = [0, 240, 480, z.deg]
    spans = list(zip(cuts[:-1], cuts[1:]))

    def left_factor(g, b):
        build_select(b)
        leg_copy(g, b).wait()
        p = order[me * z.own + g * PER + b]
        live = p < z.orders // 2
        first = jnp.where(live, z.orders - p, 0)
        second = jnp.where(live, z.orders - p, 4 * z.deg)
        in_first = marks[b, 1:2, :] == 0
        for lo, hi in spans:
            spread = jnp.dot(pbuf[lo:hi, :], sel[...], preferred_element_type=jnp.float32)
            r = lax.broadcasted_iota(jnp.int32, (hi - lo, 1), 0) + lo
            upper = jnp.where(r < first, 1.0, 0.0)
            lower = jnp.where(r >= second, 1.0, 0.0)
            mask = jnp.where(in_first, upper, lower)
            lhs[b, lo:hi, :] = (spread * mask).astype(jnp.bfloat16)

    def product(g, b):
        at = z.start[b]
        rhs = jnp.concatenate(
            [
                recv[g, :, j, at : at + z.win, :].reshape(z.depth, LANES)
                for j in range(z.nc)
            ],
            axis=1,
        )
        for lo, hi in spans:
            y = jnp.dot(lhs[b, lo:hi, :], rhs, preferred_element_type=jnp.float32)
            for t in range(z.ct):
                p0 = y[:, 2 * t * LANES : (2 * t + 1) * LANES]
                p1 = y[:, (2 * t + 1) * LANES : (2 * t + 2) * LANES]
                re = jnp.where(low, p0, pltpu.roll(p1, LANES // 2, 1))
                im = jnp.where(low, pltpu.roll(p0, LANES // 2, 1), p1)
                base = g * z.orows + (b * z.deg + lo) * z.per_row + 2 * t
                out[pl.ds(base, hi - lo, stride=z.per_row), :] = re
                out[pl.ds(base + 1, hi - lo, stride=z.per_row), :] = im

    def body(g, _):
        @pl.when(g < z.groups)
        def _():
            @pl.when(g == 0)
            def _():
                clear_pads()

            transform(g)

            @pl.when(g >= 2)
            def _():
                all_sent(lax.rem(g, 2)).wait()

            pack(g)

            @pl.when(g == 0)
            def _():
                pl.semaphore_wait(barrier, z.nd - 1)

            ship(g)

        @pl.when(g >= 2)
        def _():
            for b in range(PER):
                leg_copy(g - 2, b).start()
                left_factor(g - 2, b)
            for b in range(PER):
                all_here(g - 2, b).wait()
                product(g - 2, b)

        return 0

    lax.fori_loop(0, z.groups + 2, body, 0)
    for g in range(max(z.groups - 2, 0), z.groups):
        all_sent(g % 2).wait()


def per_device(field, legendre, pair_order):
    z = Sizes(
        field.shape, legendre.shape, lax.axis_size("lat"), lax.axis_size("ch")
    )
    held = pair_order.reshape(z.blocks, DB, z.groups, PER).transpose(2, 0, 3, 1)
    held = jnp.broadcast_to(held[:, :, :, None, :], (z.groups, z.blocks, PER, 4, DB))
    held = held.reshape(z.groups, 1, z.blocks * 8 * DB)

    col = np.arange(z.depth)
    marks = np.zeros((PER, 8, z.depth), np.int32)
    for b in range(PER):
        u = col % z.win - (b * z.pair - z.start[b])
        lat = (col // z.win) * z.rows + u % z.rows
        ok = (u >= 0) & (u < z.pair) & (lat < NLAT)
        marks[b, 0] = np.where(ok, lat, -1)
        marks[b, 1] = (u // z.rows) % 2

    bf, f32 = jnp.bfloat16, jnp.float32
    vmem = pl.BlockSpec(memory_space=pltpu.VMEM)
    hbm = pl.BlockSpec(memory_space=pl.ANY)
    dma = pltpu.SemaphoreType.DMA
    flat = pl.pallas_call(
        functools.partial(kernel, z),
        out_shape=pltpu.VMEM((z.groups * z.orows, LANES), f32),
        in_specs=[hbm, hbm, vmem, vmem, pl.BlockSpec(memory_space=pltpu.SMEM)],
        out_specs=vmem,
        scratch_shapes=[
            pltpu.VMEM((SLOTS, z.cpad, z.lon), bf),
            pltpu.VMEM((z.blocks, z.lon, 8 * DB), bf),
            pltpu.VMEM((z.nd * z.zrows, LANES), f32),
            pltpu.VMEM((2, z.nd, z.zrows, LANES), bf),
            pltpu.VMEM((z.groups, z.nl, z.nc, z.zrows, LANES), bf),
            pltpu.VMEM((z.latp, z.depth), bf),
            pltpu.VMEM((z.deg, z.latp), bf),
            pltpu.VMEM((PER, z.deg, z.depth), bf),
            dma((SLOTS,)), dma, dma((2,)), dma((z.groups, len(z.pieces))),
        ],
        compiler_params=pltpu.CompilerParams(
            collective_id=0, has_side_effects=True, vmem_limit_bytes=67043328 - 4 * LANES * z.groups * z.orows - (1 << 18)
        ),
    )(
        field.reshape(z.rows * z.chan, z.lon), legendre, held, jnp.asarray(marks), pair_order
    )
    shaped = flat.reshape(z.own, z.deg, z.ct, 2, LANES).transpose(0, 1, 3, 2, 4)
    return shaped.reshape(z.own, z.deg, 2, z.ct * LANES)


def solution(mesh):
    in_specs = (P("lat", "ch", None), P(("lat", "ch"), None, None), P())
    out_specs = P(("lat", "ch"), None, None, None)
    return jax.shard_map(
        per_device, mesh=mesh, in_specs=in_specs, out_specs=out_specs, check_vma=False
    )
```
